32 devices in a mesh: rep: 2 (over z, core), dp: 16 (over x, y).
Axes of the slice: x: 4, y: 4, z: 1, core: 2. Of those that a mesh axis runs over, the one named last changes fastest.
The devices are a block of a 4x4x8 slice.
Arguments:
- x: bfloat16 [32, 2048, 768], P(('rep', 'dp')), parts along dimension 0
- dy: bfloat16 [32, 2048, 768], P(('rep', 'dp')), parts along dimension 0
- w_gate: bfloat16 [2, 768, 2304], replicated
- w_up: bfloat16 [2, 768, 2304], replicated
- w_down: bfloat16 [2, 2304, 768], replicated
- m_w_gate: float32 [2, 768, 2304], replicated
- m_w_up: float32 [2, 768, 2304], replicated
- m_w_down: float32 [2, 2304, 768], replicated
- v_w_gate: float32 [2, 768, 2304], replicated
- v_w_up: float32 [2, 768, 2304], replicated
- v_w_down: float32 [2, 2304, 768], replicated
Outputs:
- output 1: bfloat16 [4, 768, 2304], P('rep'), parts along dimension 0
- output 2: bfloat16 [4, 768, 2304], P('rep'), parts along dimension 0
- output 3: bfloat16 [4, 2304, 768], P('rep'), parts along dimension 0
- output 4: float32 [4, 768, 2304], P('rep'), parts along dimension 0
- output 5: float32 [4, 768, 2304], P('rep'), parts along dimension 0
- output 6: float32 [4, 2304, 768], P('rep'), parts along dimension 0
- output 7: float32 [4, 768, 2304], P('rep'), parts along dimension 0
- output 8: float32 [4, 768, 2304], P('rep'), parts along dimension 0
- output 9: float32 [4, 2304, 768], P('rep'), parts along dimension 0
There are 2 independent parts. The reference program is written for one: setup_inputs(seed, part) draws one part's arguments, and reference() takes and returns one part's arrays. A program takes and returns all parts, laid end to end along the dimension named above; an argument that names none is the same for every part.
All inputs are finite; a program needn't handle non-finite values.
Results may differ from the reference program's by a relative error of at most 0.022.
Values are sent between devices in bfloat16 or wider.
A program may use at most 768 MiB of HBM per device.

```python
import jax
import jax.numpy as jnp
from jax import lax

SEQUENCES = 16
TOKENS = 2048
D = 768
FF = 2304
LAYERS = 2
NAMES = ("w_gate", "w_up", "w_down")
SHAPES = {"w_gate": (LAYERS, D, FF), "w_up": (LAYERS, D, FF), "w_down": (LAYERS, FF, D)}


def bump(key, n, height):
    away = (jnp.arange(n, dtype=jnp.int32) - jax.random.randint(key, (), 0, n, jnp.int32)) % n
    return jnp.where(away < n // 8, height, 1.0)


def together(key, own, strength):
    shared = jax.random.normal(key, own.shape[1:], jnp.float32)
    return (own + strength * shared) * lax.rsqrt(1 + strength * strength)


def setup_inputs(seed: int = 0, part: int = 0) -> dict:
    kx, kdy, ka, kb, kz, kf, kh, kl, *keys = jax.random.split(jax.random.key(seed), 8 + 3 * len(NAMES))
    kx, kdy, ka, kb = (jax.random.fold_in(k, part) for k in (kx, kdy, ka, kb))
    kw, km, kv = (keys[i::3] for i in range(3))
    shape = (SEQUENCES, TOKENS, D)
    much_x, much_dy = jax.random.uniform(kz, (2,), jnp.float32, 0.0, 1.0)
    loud = 2.0 ** jax.random.uniform(jax.random.fold_in(kz, 1), (), jnp.float32, -1.0, 2.0)
    layers = 2.0 ** jax.random.uniform(kl, (LAYERS, 1, 1), jnp.float32, -1.0, 1.0)
    x = together(ka, jax.random.normal(kx, shape, jnp.float32), much_x) * bump(kf, D, 4.0)
    dy = together(kb, jax.random.normal(kdy, shape, jnp.float32), much_dy)
    drawn = {"x": x.astype(jnp.bfloat16), "dy": (loud * dy * (SEQUENCES * TOKENS) ** -0.5).astype(jnp.bfloat16)}
    for key, name in zip(kw, NAMES, strict=True):
        w = jax.random.normal(key, SHAPES[name], jnp.float32) * SHAPES[name][1] ** -0.5
        drawn[name] = (w * {"w_gate": 1.0, "w_up": bump(kh, FF, 4.0), "w_down": layers}[name]).astype(jnp.bfloat16)
    for key, name in zip(km, NAMES, strict=True):
        drawn[f"m_{name}"] = 0.1 * jax.random.normal(key, SHAPES[name], jnp.float32)
    for key, name in zip(kv, NAMES, strict=True):
        drawn[f"v_{name}"] = jax.random.uniform(key, SHAPES[name], jnp.float32, 0.005, 0.015)
    return drawn


def matmul(a, w):
    return jnp.dot(a, w, preferred_element_type=jnp.float32).astype(jnp.bfloat16)


def normed(h):
    wide = h.astype(jnp.float32)
    scale = lax.rsqrt(jnp.mean(wide**2, -1, keepdims=True) + 1e-6)
    return (wide * scale).astype(jnp.bfloat16)


def layer(h, w):
    a = normed(h)
    gate = jnp.dot(a, w["w_gate"], preferred_element_type=jnp.float32)
    up = jnp.dot(a, w["w_up"], preferred_element_type=jnp.float32)
    return h + matmul((jax.nn.silu(gate) * up).astype(jnp.bfloat16), w["w_down"])


def adamw(w, m, v, g):
    m = 0.9 * m + 0.1 * g
    v = 0.95 * v + 0.05 * g * g
    step = m * lax.rsqrt(v + 1e-8) + 0.1 * w
    return (w - 0.02 * step).astype(jnp.bfloat16), m, v


def clipped(gradients, sum_of_squares, count):
    factor = jnp.minimum(1.0, 0.5 * lax.rsqrt(sum_of_squares / count + 1e-30))
    return [g * factor for g in gradients]


def stack(weights, h):
    return lax.scan(lambda h, w: (layer(h, w), None), h, weights)[0]


def reference(x, dy, w_gate, w_up, w_down, m_w_gate, m_w_up, m_w_down, v_w_gate, v_w_up, v_w_down):
    weights = dict(zip(NAMES, (w_gate, w_up, w_down), strict=True))

    def take(so_far, sequence):
        h, by_y = sequence
        _, back = jax.vjp(lambda w: stack(w, h), weights)
        return jax.tree.map(lambda total, term: total + term.astype(jnp.float32), so_far, back(by_y)[0]), None

    none_yet = {name: jnp.zeros(w.shape, jnp.float32) for name, w in weights.items()}
    by_weights, _ = lax.scan(take, none_yet, (x, dy))
    gradients = [by_weights[name].astype(jnp.bfloat16).astype(jnp.float32) for name in NAMES]
    gradients = clipped(gradients, sum(jnp.sum(g * g) for g in gradients), sum(g.size for g in gradients))
    new = [
        adamw(w.astype(jnp.float32), m, v, g)
        for w, m, v, g in zip((w_gate, w_up, w_down), (m_w_gate, m_w_up, m_w_down), (v_w_gate, v_w_up, v_w_down), gradients, strict=True)
    ]
    return tuple(one[which] for which in range(3) for one in new)
```

```python
import functools
import math

import jax
import jax.numpy as jnp
from jax import lax
from jax.experimental import pallas as pl
from jax.experimental.pallas import tpu as pltpu
from jax.sharding import PartitionSpec as P

MESH = pl.DeviceIdType.MESH
F32, BF16 = jnp.float32, jnp.bfloat16
BLOCK = 256
ROWS = 256
LANES = 128
OWN_SLOTS, RECV_SLOTS, SEND_SLOTS, KEEP_SLOTS, PUT_SLOTS = 8, 3, 2, 4, 4
COLOURS = ((0, 1), (0, -1), (1, 1), (1, -1))


def dot(a, b):
    return jnp.dot(a, b, preferred_element_type=F32)


def dot_t(a, b):
    return lax.dot_general(a, b, (((1,), (1,)), ((), ())), preferred_element_type=F32)


def step_kernel(dims, x_ref, dy_ref, wg_ref, wu_ref, wd_ref, shard_ref, square_ref, whole_ref,
                squares, h, a, a_t, ct, ct_t, acc, wg, wu, wd, p_gate, p_up, p_prod, own, r1, r2, s1, s2, keep,
                w_sem, io_sem, send_sem, recv_sem, put_sem, square_send, square_recv):
    side, gathered, layers, tokens, d, ff = dims
    blocks = ff // BLOCK
    units = layers * blocks
    forward = (layers - 1) * blocks
    unit_rows = own.shape[1]
    colour_rows = unit_rows // len(COLOURS)
    chunk, sub = colour_rows // side, colour_rows // (side * side)
    hops = side - 1
    steps = 2 * hops

    me = lax.axis_index("dp")
    place = (me // side, me % side)

    def neighbour(axis, by):
        at = list(place)
        at[axis] = lax.rem(at[axis] + by + side, side)
        return {"dp": at[0] * side + at[1]}

    peers = side * side
    barrier = pltpu.get_barrier_semaphore()
    for away in range(1, peers):
        pl.semaphore_signal(barrier, inc=1, device_id={"dp": lax.rem(me + away, peers)}, device_id_type=MESH)

    def weights(n):
        slot = lax.rem(n, 2)
        back = n - forward
        layer = jnp.where(n < forward, n // blocks, layers - 1 - back // blocks)
        at = pl.ds(pl.multiple_of(lax.rem(n, blocks) * BLOCK, BLOCK), BLOCK)
        return [
            pltpu.make_async_copy(wg_ref.at[layer, :, at], wg.at[slot], w_sem.at[slot, 0]),
            pltpu.make_async_copy(wu_ref.at[layer, :, at], wu.at[slot], w_sem.at[slot, 1]),
            pltpu.make_async_copy(wd_ref.at[layer, at, :], wd.at[slot], w_sem.at[slot, 2]),
        ]

    def next_weights(n):
        for copy in weights(n):
            copy.wait()

        @pl.when(n + 1 < forward + units)
        def _():
            for copy in weights(n + 1):
                copy.start()

    load_x, load_dy = (pltpu.make_async_copy(ref.at[0], ct, io_sem.at[i]) for i, ref in enumerate((x_ref, dy_ref)))
    load_x.start()
    for copy in weights(0):
        copy.start()

    tiles = [slice(at, at + ROWS) for at in range(0, tokens, ROWS)]

    def into(layer, rows):
        return ct[rows] if layer == 0 else h[layer - 1, rows]

    def norm_of(layer, rows):
        wide = into(layer, rows).astype(F32)
        scale = lax.rsqrt(jnp.mean(wide * wide, -1, keepdims=True) + 1e-6)
        return wide, scale

    def norm(layer):
        for rows in tiles:
            wide, scale = norm_of(layer, rows)
            out = (wide * scale).astype(BF16)
            a[layer, rows] = out
            a_t[layer, :, rows] = out.T

    load_x.wait()
    norm(0)

    for layer in range(layers - 1):
        acc[...] = jnp.zeros_like(acc)

        def forward_block(j, _, layer=layer):
            n = layer * blocks + j
            next_weights(n)
            slot = lax.rem(n, 2)
            for rows in tiles:
                at = a[layer, rows]
                gate, up = dot(at, wg[slot]), dot(at, wu[slot])
                prod = (gate * jax.nn.sigmoid(gate) * up).astype(BF16)
                acc[rows] += dot(prod, wd[slot])
            return 0

        lax.fori_loop(0, blocks, forward_block, 0)
        for rows in tiles:
            h[layer, rows] = into(layer, rows) + acc[rows].astype(BF16)
        if layer == 0:
            load_dy.start()
        norm(layer + 1)
    load_dy.wait()
    for rows in tiles:
        ct_t[:, rows] = ct[rows].T

    def copy_of(k, s, c, source):
        first, by = COLOURS[c]
        axis = first if s < hops else 1 - first
        slot = lax.rem(k, RECV_SLOTS)
        target = r1.at[slot, c, s] if s < hops else r2.at[slot, c, s - hops]
        return pltpu.make_async_remote_copy(
            src_ref=source, dst_ref=target, send_sem=send_sem.at[lax.rem(k, SEND_SLOTS), c, s],
            recv_sem=recv_sem.at[slot, c, s], device_id=neighbour(axis, by), device_id_type=MESH)

    def own_rows(c, s):
        first, by = COLOURS[c]
        q = lax.rem(place[first] - by * (1 + s) + 2 * side, side)
        return pl.ds(pl.multiple_of(c * colour_rows + q * chunk, chunk), chunk)

    def sub_at(c, t):
        first, by = COLOURS[c]
        return lax.rem(place[1 - first] - by * (1 + t) + 2 * side, side)

    def source_of(k, s, c):
        if s == 0:
            return own.at[lax.rem(k - 1, OWN_SLOTS), own_rows(c, 0)]
        if s < hops:
            return s1.at[lax.rem(k, SEND_SLOTS), c, s - 1]
        return s2.at[lax.rem(k, SEND_SLOTS), c, s - hops]

    def spread_rows(c, s):
        first, by = COLOURS[c]
        if s < hops:
            q, r = place[first], lax.rem(place[1 - first] - by * s + side, side)
            return pl.ds(pl.multiple_of(c * colour_rows + q * chunk + r * sub, 8), sub)
        q = lax.rem(place[first] - by * (s - hops) + side, side)
        return pl.ds(pl.multiple_of(c * colour_rows + q * chunk, chunk), chunk)

    def spread(k, s, c, p):
        first, by = COLOURS[c]
        axis = 1 - first if s < hops else first
        target = whole_ref.at[p, spread_rows(c, s)]
        return pltpu.make_async_remote_copy(
            src_ref=shard_ref.at[p, c] if s == 0 else target, dst_ref=target,
            send_sem=send_sem.at[lax.rem(k, SEND_SLOTS), c, steps + s], recv_sem=recv_sem.at[lax.rem(k, RECV_SLOTS), c, steps + s],
            device_id=neighbour(axis, by), device_id_type=MESH)

    def put(c, p):
        return pltpu.make_async_copy(shard_ref.at[p, c], whole_ref.at[p, spread_rows(c, 0)], put_sem.at[lax.rem(p, PUT_SLOTS), c])

    def within(p, last):
        return (p >= 0) & (p < last)

    def gather_step(k, s):
        p = k - 1 - steps - s
        safe = jnp.clip(p, 0, units - 1)
        if s < steps:
            @pl.when(within(p - SEND_SLOTS, gathered))
            def _():
                for c in range(len(COLOURS)):
                    spread(k, s, c, jnp.clip(p - SEND_SLOTS, 0, units - 1)).wait_send()

        @pl.when(within(p, gathered))
        def _():
            for c in range(len(COLOURS)):
                if s >= 1:
                    spread(k + RECV_SLOTS - 1, s - 1, c, safe).wait_recv()
                if s == hops:
                    put(c, safe).wait()
                if s < steps:
                    spread(k, s, c, safe).start()
                if s == 0:
                    put(c, safe).start()

    def sum_step(k, s):
        was, now = lax.rem(k + RECV_SLOTS - 1, RECV_SLOTS), lax.rem(k, SEND_SLOTS)
        p = k - 1 - s
        if s < steps:
            @pl.when(within(p - SEND_SLOTS, units))
            def _():
                for c in range(len(COLOURS)):
                    copy_of(k, s, c, source_of(k, s, c)).wait_send()

        @pl.when(within(p, units))
        def _():
            mine, kept = lax.rem(p + 2 * OWN_SLOTS, OWN_SLOTS), lax.rem(p + 2 * KEEP_SLOTS, KEEP_SLOTS)
            for c in range(len(COLOURS)):
                if s >= 1:
                    copy_of(k + RECV_SLOTS - 1, s - 1, c, source_of(k, s - 1, c)).wait_recv()
                if 1 <= s < hops:
                    s1[now, c, s - 1] = (r1[was, c, s - 1].astype(F32) + own[mine, own_rows(c, s)].astype(F32)).astype(BF16)
                elif s == hops:
                    total = r1[was, c, s - 1].astype(F32) + own[mine, own_rows(c, s)].astype(F32)
                    for i in range(side):
                        keep[kept, c, i] = total[i * sub : (i + 1) * sub]
                    s2[now, c, 0] = keep[kept, c, sub_at(c, 0)].astype(BF16)
                elif hops < s < steps:
                    t = s - hops
                    s2[now, c, t] = (r2[was, c, t - 1].astype(F32) + keep[kept, c, sub_at(c, t)]).astype(BF16)
                elif s == steps:
                    total = (r2[was, c, hops - 1].astype(F32) + keep[kept, c, sub_at(c, hops)]).astype(BF16)
                    shard_ref[p, c] = total
                    wide = total.astype(F32)
                    squares[me] += jnp.sum((wide * wide).reshape(sub // 8, 8, LANES), 0)
            if s < steps:
                for c in range(len(COLOURS)):
                    copy_of(k, s, c, source_of(k, s, c)).start()

    def communicate(k):
        for s in range(steps, 0, -1):
            gather_step(k, s)
        sum_step(k, steps)
        gather_step(k, 0)
        for s in range(steps - 1, -1, -1):
            sum_step(k, s)

    squares[me] = jnp.zeros((8, LANES), F32)
    pl.semaphore_wait(barrier, peers - 1)

    for back in range(layers):
        layer = layers - 1 - back
        if layer > 0:
            acc[...] = jnp.zeros_like(acc)

        def unit(j, _, layer=layer, back=back):
            k = back * blocks + j
            communicate(k)
            next_weights(forward + k)
            slot, mine = lax.rem(forward + k, 2), lax.rem(k, OWN_SLOTS)
            for rows in tiles:
                at = a[layer, rows]
                gate, up = dot(at, wg[slot]), dot(at, wu[slot])
                by_prod = dot_t(ct[rows], wd[slot]).astype(BF16).astype(F32)
                sig = jax.nn.sigmoid(gate)
                silu = gate * sig
                p_prod[rows] = (silu * up).astype(BF16)
                p_up[rows] = (by_prod * silu).astype(BF16)
                p_gate[rows] = (by_prod * up * (sig + silu * (1 - sig))).astype(BF16)
            at = 0
            for which in (p_gate, p_up):
                g = dot(a_t[layer], which[...]).astype(BF16)
                for i in range(BLOCK // LANES):
                    own[mine, at : at + d] = g[:, i * LANES : (i + 1) * LANES]
                    at += d
            g = dot(ct_t[...], p_prod[...]).astype(BF16).T
            for i in range(d // LANES):
                own[mine, at : at + BLOCK] = g[:, i * LANES : (i + 1) * LANES]
                at += BLOCK
            if layer > 0:
                for rows in tiles:
                    acc[rows] += dot_t(p_gate[rows], wg[slot]) + dot_t(p_up[rows], wu[slot])
            return 0

        lax.fori_loop(0, blocks, unit, 0)
        if layer > 0:
            for rows in tiles:
                wide, scale = norm_of(layer, rows)
                by_a = acc[rows].astype(BF16).astype(F32)
                by_h = by_a * scale - wide * (scale * scale * scale * jnp.mean(by_a * wide, -1, keepdims=True))
                new = ct[rows] + by_h.astype(BF16)
                ct[rows] = new
                ct_t[:, rows] = new.T

    def drain(k, _):
        communicate(k)
        return 0

    done = units + steps + 1
    lax.fori_loop(units, done, drain, 0)

    def square_to(away):
        return pltpu.make_async_remote_copy(
            src_ref=squares.at[me], dst_ref=squares.at[me], send_sem=square_send.at[away], recv_sem=square_recv.at[me],
            device_id={"dp": lax.rem(me + away, peers)}, device_id_type=MESH)

    for away in range(1, peers):
        square_to(away).start()
    lax.fori_loop(done, max(done + 1, gathered + 2 * steps + 2), drain, 0)
    for away in range(1, peers):
        square_to(away).wait_send()
        other = lax.rem(me + away, peers)
        pltpu.make_async_remote_copy(
            src_ref=squares.at[other], dst_ref=squares.at[other], send_sem=square_send.at[away], recv_sem=square_recv.at[other],
            device_id={"dp": other}, device_id_type=MESH).wait_recv()
    total = squares[0]
    for i in range(1, peers):
        total = total + squares[i]
    square_ref[...] = total


def gradients(n, gathered, x, dy, w_gate, w_up, w_down):
    side = math.isqrt(n)
    layers, d, ff = w_gate.shape
    tokens = x.shape[1]
    units, unit_rows = layers * (ff // BLOCK), 3 * d * BLOCK // LANES
    colours = len(COLOURS)
    chunk, sub = unit_rows // (colours * side), unit_rows // (colours * side * side)
    hops = side - 1
    dims = (side, gathered, layers, tokens, d, ff)
    any_space, vmem = pl.BlockSpec(memory_space=pl.ANY), pl.BlockSpec(memory_space=pltpu.VMEM)
    return pl.pallas_call(
        functools.partial(step_kernel, dims),
        out_shape=(
            jax.ShapeDtypeStruct((units, colours, sub, LANES), BF16),
            jax.ShapeDtypeStruct((8, LANES), F32),
            jax.ShapeDtypeStruct((gathered, unit_rows, LANES), BF16),
        ),
        in_specs=[any_space] * 5,
        out_specs=(vmem, vmem, any_space),
        scratch_shapes=[
            pltpu.VMEM((n, 8, LANES), F32),
            pltpu.VMEM((layers - 1, tokens, d), BF16),
            pltpu.VMEM((layers, tokens, d), BF16),
            pltpu.VMEM((layers, d, tokens), BF16),
            pltpu.VMEM((tokens, d), BF16),
            pltpu.VMEM((d, tokens), BF16),
            pltpu.VMEM((tokens, d), F32),
            pltpu.VMEM((2, d, BLOCK), BF16),
            pltpu.VMEM((2, d, BLOCK), BF16),
            pltpu.VMEM((2, BLOCK, d), BF16),
            pltpu.VMEM((tokens, BLOCK), BF16),
            pltpu.VMEM((tokens, BLOCK), BF16),
            pltpu.VMEM((tokens, BLOCK), BF16),
            pltpu.VMEM((OWN_SLOTS, unit_rows, LANES), BF16),
            pltpu.VMEM((RECV_SLOTS, colours, hops, chunk, LANES), BF16),
            pltpu.VMEM((RECV_SLOTS, colours, hops, sub, LANES), BF16),
            pltpu.VMEM((SEND_SLOTS, colours, hops - 1, chunk, LANES), BF16),
            pltpu.VMEM((SEND_SLOTS, colours, hops, sub, LANES), BF16),
            pltpu.VMEM((KEEP_SLOTS, colours, side, sub, LANES), F32),
            pltpu.SemaphoreType.DMA((2, 3)),
            pltpu.SemaphoreType.DMA((2,)),
            pltpu.SemaphoreType.DMA((SEND_SLOTS, colours, 4 * hops)),
            pltpu.SemaphoreType.DMA((RECV_SLOTS, colours, 4 * hops)),
            pltpu.SemaphoreType.DMA((PUT_SLOTS, colours)),
            pltpu.SemaphoreType.DMA((n,)),
            pltpu.SemaphoreType.DMA((n,)),
        ],
        compiler_params=pltpu.CompilerParams(collective_id=0, has_side_effects=True, vmem_limit_bytes=67043328),
    )(x, dy, w_gate, w_up, w_down)


def update_kernel(runs, factor_ref, g_ref, *refs):
    ins, outs = refs[:9], refs[9:]
    factor = factor_ref[0, 0]
    for which, rows, cols, at in runs:
        g = g_ref[0, at].astype(F32) * factor
        m = 0.9 * ins[3 + which][0, rows, cols] + 0.1 * g
        v = 0.95 * ins[6 + which][0, rows, cols] + 0.05 * g * g
        w = ins[which][0, rows, cols].astype(F32)
        outs[which][0, rows, cols] = (w - 0.02 * (m * lax.rsqrt(v + 1e-8) + 0.1 * w)).astype(BF16)
        outs[3 + which][0, rows, cols] = m
        outs[6 + which][0, rows, cols] = v


def update(factor, g, arrays):
    layers, d, ff = arrays[0].shape
    blocks = ff // BLOCK
    runs, at = [], 0
    for which, height, width in ((0, d, BLOCK), (1, d, BLOCK), (2, BLOCK, d)):
        for i in range(width // LANES):
            for top in range(0, height, 64):
                runs.append((which, slice(top, top + 64), slice(i * LANES, (i + 1) * LANES), slice(at, at + 64)))
                at += 64

    def wide(u):
        return layers - 1 - u // blocks, 0, u % blocks

    def tall(u):
        return layers - 1 - u // blocks, u % blocks, 0

    specs = [pl.BlockSpec((1, d, BLOCK), wide), pl.BlockSpec((1, d, BLOCK), wide), pl.BlockSpec((1, BLOCK, d), tall)] * 3
    return pl.pallas_call(
        functools.partial(update_kernel, runs),
        grid=(layers * blocks,),
        out_shape=tuple(jax.ShapeDtypeStruct(a.shape, a.dtype) for a in arrays),
        in_specs=[pl.BlockSpec(memory_space=pltpu.SMEM), pl.BlockSpec((1, g.shape[1], LANES), lambda u: (u, 0, 0))] + specs,
        out_specs=tuple(specs),
        compiler_params=pltpu.CompilerParams(vmem_limit_bytes=50 * 2**20),
    )(factor, g, *arrays)


def solution(mesh):
    n = mesh.shape["dp"]

    def step(x, dy, *arrays):
        layers, d, ff = arrays[0].shape
        units = layers * (ff // BLOCK)
        shards, squares, whole = gradients(n, units, x, dy, *arrays[:3])
        count = sum(w.size for w in arrays[:3])
        factor = jnp.minimum(1.0, 0.5 * lax.rsqrt(jnp.sum(squares) / count + 1e-30))
        return update(factor.reshape(1, 1), whole, arrays)

    return jax.shard_map(
        step,
        mesh=mesh,
        in_specs=(P(("rep", "dp"), None, None),) * 2 + (P(None, None, None),) * 9,
        out_specs=(P("rep", None, None),) * 9,
        check_vma=False,
    )
```

```python
import functools
import math

import jax
import jax.numpy as jnp
from jax import lax
from jax.experimental import pallas as pl
from jax.experimental.pallas import tpu as pltpu
from jax.sharding import PartitionSpec as P

MESH = pl.DeviceIdType.MESH
F32, BF16 = jnp.float32, jnp.bfloat16
BLOCK = 256
ROWS = 512
LANES = 128
OWN_SLOTS, RECV_SLOTS, SEND_SLOTS, KEEP_SLOTS, PUT_SLOTS = 5, 3, 2, 4, 4
SCRATCHES = 27
GROUPS = (((0, 0), (1, 0), (2, 0), (3, 0), (0, 1), (1, 1)), ((2, 1), (3, 1), (0, 2), (1, 2), (2, 2), (3, 2)), ((0, 3), (1, 3), (2, 3), (3, 3)))
UPDATE_SLOTS = 4
INSIDE = 1
COLOURS = ((0, 1), (0, -1), (1, 1), (1, -1))


def dot(a, b):
    return jnp.dot(a, b, preferred_element_type=F32)


def dot_t(a, b):
    return lax.dot_general(a, b, (((1,), (1,)), ((), ())), preferred_element_type=F32)


def step_kernel(dims, x_ref, dy_ref, wg_ref, wu_ref, wd_ref, shard_ref, factor_ref, *refs):
    parts, (squares, x, h, a, a_t, ct, ct_t, acc, wg, wu, wd, p_gate, p_up, p_prod, own, r1, r2, s1, s2, keep,
            w_sem, io_sem, send_sem, recv_sem, put_sem, square_send, square_recv) = refs[: -SCRATCHES], refs[-SCRATCHES:]
    side, layers, tokens, d, ff = dims
    parts = [parts[i : i + len(COLOURS)] for i in range(0, len(parts), len(COLOURS))]
    blocks = ff // BLOCK
    units = layers * blocks
    forward = (layers - 1) * blocks
    unit_rows = own.shape[1]
    colour_rows = unit_rows // len(COLOURS)
    chunk, sub = colour_rows // side, colour_rows // (side * side)
    hops = side - 1
    steps = 2 * hops
    spreads = hops + len(parts) - 1

    me = lax.axis_index("dp")
    place = (me // side, me % side)

    def neighbour(axis, by):
        at = list(place)
        at[axis] = lax.rem(at[axis] + by + side, side)
        return {"dp": at[0] * side + at[1]}

    peers = side * side
    barrier = pltpu.get_barrier_semaphore()
    for away in range(1, peers):
        pl.semaphore_signal(barrier, inc=1, device_id={"dp": lax.rem(me + away, peers)}, device_id_type=MESH)

    def weights(n):
        slot = lax.rem(n, 2)
        back = n - forward
        layer = jnp.where(n < forward, n // blocks, layers - 1 - back // blocks)
        at = pl.ds(pl.multiple_of(lax.rem(n, blocks) * BLOCK, BLOCK), BLOCK)
        return [
            pltpu.make_async_copy(wg_ref.at[layer, :, at], wg.at[slot], w_sem.at[slot, 0]),
            pltpu.make_async_copy(wu_ref.at[layer, :, at], wu.at[slot], w_sem.at[slot, 1]),
            pltpu.make_async_copy(wd_ref.at[layer, at, :], wd.at[slot], w_sem.at[slot, 2]),
        ]

    def next_weights(n):
        for copy in weights(n):
            copy.wait()

        @pl.when(n + 1 < forward + units)
        def _():
            for copy in weights(n + 1):
                copy.start()

    load_x, load_dy = (pltpu.make_async_copy(ref.at[0], to, io_sem.at[i]) for i, (ref, to) in enumerate(((x_ref, x), (dy_ref, ct))))
    load_x.start()
    load_dy.start()
    for copy in weights(0):
        copy.start()

    tiles = [slice(at, at + ROWS) for at in range(0, tokens, ROWS)]

    def into(layer, rows):
        return x[rows] if layer == 0 else h[layer - 1, rows]

    def norm_of(layer, rows):
        wide = into(layer, rows).astype(F32)
        scale = lax.rsqrt(jnp.mean(wide * wide, -1, keepdims=True) + 1e-6)
        return wide, scale

    def norm(layer):
        for rows in tiles:
            wide, scale = norm_of(layer, rows)
            out = (wide * scale).astype(BF16)
            a[layer, rows] = out
            if layer == layers - 1:
                a_t[layer, :, rows] = out.T

    load_x.wait()
    norm(0)
    load_dy.wait()

    for layer in range(layers - 1):
        acc[...] = jnp.zeros_like(acc)

        def forward_block(j, _, layer=layer):
            n = layer * blocks + j
            next_weights(n)
            slot = lax.rem(n, 2)
            for rows in tiles:
                at = a[layer, rows]
                gate, up = dot(at, wg[slot]), dot(at, wu[slot])
                prod = (gate * jax.nn.sigmoid(gate) * up).astype(BF16)
                acc[rows] += dot(prod, wd[slot])
            width = tokens // (blocks - 1)
            piece = pl.ds(pl.multiple_of(jnp.minimum(j, blocks - 2) * width, width), width)
            a_t[layer, :, piece] = a[layer, piece].T
            if layer == 0:
                ct_t[:, piece] = ct[piece].T
            return 0

        lax.fori_loop(0, blocks, forward_block, 0)
        for rows in tiles:
            h[layer, rows] = into(layer, rows) + acc[rows].astype(BF16)
        norm(layer + 1)

    def copy_of(k, s, c, source):
        first, by = COLOURS[c]
        axis = first if s < hops else 1 - first
        slot = lax.rem(k, RECV_SLOTS)
        target = r1.at[slot, c, s] if s < hops else r2.at[slot, c, s - hops]
        return pltpu.make_async_remote_copy(
            src_ref=source, dst_ref=target, send_sem=send_sem.at[lax.rem(k, SEND_SLOTS), c, s],
            recv_sem=recv_sem.at[slot, c, s], device_id=neighbour(axis, by), device_id_type=MESH)

    def own_rows(c, s):
        first, by = COLOURS[c]
        q = lax.rem(place[first] - by * (1 + s) + 2 * side, side)
        return pl.ds(pl.multiple_of(c * colour_rows + q * chunk, chunk), chunk)

    def sub_at(c, t):
        first, by = COLOURS[c]
        return lax.rem(place[1 - first] - by * (1 + t) + 2 * side, side)

    def source_of(k, s, c):
        if s == 0:
            return own.at[lax.rem(k - 1, OWN_SLOTS), own_rows(c, 0)]
        if s < hops:
            return s1.at[lax.rem(k, SEND_SLOTS), c, s - 1]
        return s2.at[lax.rem(k, SEND_SLOTS), c, s - hops]

    def spread(k, s, c, p):
        first, by = COLOURS[c]
        if s < hops:
            axis, source = 1 - first, shard_ref.at[p, c] if s == 0 else parts[0][c].at[p, spread_rows(c, s)]
            target = parts[0][c].at[p, spread_rows(c, s)]
        else:
            axis, source, target = first, parts[s - hops][c].at[p], parts[s - hops + 1][c].at[p]
        return pltpu.make_async_remote_copy(
            src_ref=source, dst_ref=target,
            send_sem=send_sem.at[lax.rem(k, SEND_SLOTS), c, steps + s], recv_sem=recv_sem.at[lax.rem(k, RECV_SLOTS), c, steps + s],
            device_id=neighbour(axis, by), device_id_type=MESH)

    def spread_rows(c, s):
        first, by = COLOURS[c]
        r = lax.rem(place[1 - first] - by * s + side, side)
        return pl.ds(pl.multiple_of(r * sub, 8), sub)

    def put(c, p):
        return pltpu.make_async_copy(shard_ref.at[p, c], parts[0][c].at[p, spread_rows(c, 0)], put_sem.at[lax.rem(p, PUT_SLOTS), c])

    def within(p, last):
        return (p >= 0) & (p < last)

    def gather_step(k, s):
        p = k - 1 - steps - s
        safe = jnp.clip(p, 0, units - 1)
        if s < spreads:
            @pl.when(within(p - SEND_SLOTS, units))
            def _():
                for c in range(len(COLOURS)):
                    spread(k, s, c, jnp.clip(p - SEND_SLOTS, 0, units - 1)).wait_send()

        @pl.when(within(p, units))
        def _():
            for c in range(len(COLOURS)):
                if s >= 1:
                    spread(k + RECV_SLOTS - 1, s - 1, c, safe).wait_recv()
                if s == hops:
                    put(c, safe).wait()
                if s < spreads:
                    spread(k, s, c, safe).start()
                if s == 0:
                    put(c, safe).start()

    def sum_step(k, s):
        was, now = lax.rem(k + RECV_SLOTS - 1, RECV_SLOTS), lax.rem(k, SEND_SLOTS)
        p = k - 1 - s
        if s < steps:
            @pl.when(within(p - SEND_SLOTS, units))
            def _():
                for c in range(len(COLOURS)):
                    copy_of(k, s, c, source_of(k, s, c)).wait_send()

        @pl.when(within(p, units))
        def _():
            mine, kept = lax.rem(p + 2 * OWN_SLOTS, OWN_SLOTS), lax.rem(p + 2 * KEEP_SLOTS, KEEP_SLOTS)
            for c in range(len(COLOURS)):
                if s >= 1:
                    copy_of(k + RECV_SLOTS - 1, s - 1, c, source_of(k, s - 1, c)).wait_recv()
                if 1 <= s < hops:
                    s1[now, c, s - 1] = (r1[was, c, s - 1].astype(F32) + own[mine, own_rows(c, s)].astype(F32)).astype(BF16)
                elif s == hops:
                    total = r1[was, c, s - 1].astype(F32) + own[mine, own_rows(c, s)].astype(F32)
                    for i in range(side):
                        keep[kept, c, i] = total[i * sub : (i + 1) * sub]
                    s2[now, c, 0] = keep[kept, c, sub_at(c, 0)].astype(BF16)
                elif hops < s < steps:
                    t = s - hops
                    s2[now, c, t] = (r2[was, c, t - 1].astype(F32) + keep[kept, c, sub_at(c, t)]).astype(BF16)
                elif s == steps:
                    total = (r2[was, c, hops - 1].astype(F32) + keep[kept, c, sub_at(c, hops)]).astype(BF16)
                    shard_ref[p, c] = total
                    wide = total.astype(F32)
                    squares[me] += jnp.sum((wide * wide).reshape(sub // 8, 8, LANES), 0)
            if s < steps:
                for c in range(len(COLOURS)):
                    copy_of(k, s, c, source_of(k, s, c)).start()

    def communicate(k):
        for s in range(spreads, 0, -1):
            gather_step(k, s)
        sum_step(k, steps)
        gather_step(k, 0)
        for s in range(steps - 1, -1, -1):
            sum_step(k, s)

    squares[me] = jnp.zeros((8, LANES), F32)
    pl.semaphore_wait(barrier, peers - 1)

    for back in range(layers):
        layer = layers - 1 - back
        if layer > 0:
            acc[...] = jnp.zeros_like(acc)

        def unit(j, _, layer=layer, back=back):
            k = back * blocks + j
            communicate(k)
            next_weights(forward + k)
            slot, mine = lax.rem(forward + k, 2), lax.rem(k, OWN_SLOTS)
            for rows in tiles:
                at = a[layer, rows]
                gate, up = dot(at, wg[slot]), dot(at, wu[slot])
                by_prod = dot_t(ct[rows], wd[slot]).astype(BF16).astype(F32)
                sig = jax.nn.sigmoid(gate)
                silu = gate * sig
                p_prod[rows] = (silu * up).astype(BF16)
                p_up[rows] = (by_prod * silu).astype(BF16)
                p_gate[rows] = (by_prod * up * (sig + silu * (1 - sig))).astype(BF16)
            chunks = len(COLOURS) * side
            at, tall, low = 0, d // chunks, BLOCK // chunks
            for which in (p_gate, p_up):
                g = dot(a_t[layer], which[...]).astype(BF16)
                for i in range(BLOCK // LANES):
                    for m in range(chunks):
                        own[mine, m * chunk + at : m * chunk + at + tall] = g[m * tall : (m + 1) * tall, i * LANES : (i + 1) * LANES]
                    at += tall
            g = dot(ct_t[...], p_prod[...]).astype(BF16).T
            for i in range(d // LANES):
                for m in range(chunks):
                    own[mine, m * chunk + at : m * chunk + at + low] = g[m * low : (m + 1) * low, i * LANES : (i + 1) * LANES]
                at += low
            if layer > 0:
                for rows in tiles:
                    acc[rows] += dot_t(p_gate[rows], wg[slot]) + dot_t(p_up[rows], wu[slot])
            return 0

        lax.fori_loop(0, blocks, unit, 0)
        if layer > 0:
            for rows in tiles:
                wide, scale = norm_of(layer, rows)
                by_a = acc[rows].astype(BF16).astype(F32)
                by_h = by_a * scale - wide * (scale * scale * scale * jnp.mean(by_a * wide, -1, keepdims=True))
                new = ct[rows] + by_h.astype(BF16)
                ct[rows] = new
                ct_t[:, rows] = new.T

    def drain(k, _):
        communicate(k)
        return 0

    done = units + steps + 1
    lax.fori_loop(units, done, drain, 0)

    def square_to(away):
        return pltpu.make_async_remote_copy(
            src_ref=squares.at[me], dst_ref=squares.at[me], send_sem=square_send.at[away], recv_sem=square_recv.at[me],
            device_id={"dp": lax.rem(me + away, peers)}, device_id_type=MESH)

    for away in range(1, peers):
        square_to(away).start()
    lax.fori_loop(done, units + steps + spreads + SEND_SLOTS, drain, 0)
    for away in range(1, peers):
        square_to(away).wait_send()
        other = lax.rem(me + away, peers)
        pltpu.make_async_remote_copy(
            src_ref=squares.at[other], dst_ref=squares.at[other], send_sem=square_send.at[away], recv_sem=square_recv.at[other],
            device_id={"dp": other}, device_id_type=MESH).wait_recv()
    total = squares[0]
    for i in range(1, peers):
        total = total + squares[i]
    mean = jnp.sum(total, keepdims=True) / (3 * layers * d * ff)
    factor_ref[...] = jnp.broadcast_to(jnp.minimum(1.0, 0.5 * lax.rsqrt(mean + 1e-30)), factor_ref.shape)


def gradients(n, x, dy, w_gate, w_up, w_down):
    side = math.isqrt(n)
    layers, d, ff = w_gate.shape
    tokens = x.shape[1]
    units, unit_rows = layers * (ff // BLOCK), 3 * d * BLOCK // LANES
    colours = len(COLOURS)
    chunk, sub = unit_rows // (colours * side), unit_rows // (colours * side * side)
    hops = side - 1
    dims = (side, layers, tokens, d, ff)
    any_space, vmem = pl.BlockSpec(memory_space=pl.ANY), pl.BlockSpec(memory_space=pltpu.VMEM)
    return pl.pallas_call(
        functools.partial(step_kernel, dims),
        out_shape=(
            jax.ShapeDtypeStruct((units, colours, sub, LANES), BF16),
            jax.ShapeDtypeStruct((8, LANES), F32),
            *[jax.ShapeDtypeStruct((units, chunk, LANES), BF16)] * (colours * (INSIDE + 1)),
        ),
        in_specs=[any_space] * 5,
        out_specs=(vmem, vmem, *[any_space] * (colours * (INSIDE + 1))),
        scratch_shapes=[
            pltpu.VMEM((n, 8, LANES), F32),
            pltpu.VMEM((tokens, d), BF16),
            pltpu.VMEM((layers - 1, tokens, d), BF16),
            pltpu.VMEM((layers, tokens, d), BF16),
            pltpu.VMEM((layers, d, tokens), BF16),
            pltpu.VMEM((tokens, d), BF16),
            pltpu.VMEM((d, tokens), BF16),
            pltpu.VMEM((tokens, d), F32),
            pltpu.VMEM((2, d, BLOCK), BF16),
            pltpu.VMEM((2, d, BLOCK), BF16),
            pltpu.VMEM((2, BLOCK, d), BF16),
            pltpu.VMEM((tokens, BLOCK), BF16),
            pltpu.VMEM((tokens, BLOCK), BF16),
            pltpu.VMEM((tokens, BLOCK), BF16),
            pltpu.VMEM((OWN_SLOTS, unit_rows, LANES), BF16),
            pltpu.VMEM((RECV_SLOTS, colours, hops, chunk, LANES), BF16),
            pltpu.VMEM((RECV_SLOTS, colours, hops, sub, LANES), BF16),
            pltpu.VMEM((SEND_SLOTS, colours, hops - 1, chunk, LANES), BF16),
            pltpu.VMEM((SEND_SLOTS, colours, hops, sub, LANES), BF16),
            pltpu.VMEM((KEEP_SLOTS, colours, side, sub, LANES), F32),
            pltpu.SemaphoreType.DMA((2, 3)),
            pltpu.SemaphoreType.DMA((2,)),
            pltpu.SemaphoreType.DMA((SEND_SLOTS, colours, 4 * hops)),
            pltpu.SemaphoreType.DMA((RECV_SLOTS, colours, 4 * hops)),
            pltpu.SemaphoreType.DMA((PUT_SLOTS, colours)),
            pltpu.SemaphoreType.DMA((n,)),
            pltpu.SemaphoreType.DMA((n,)),
        ],
        compiler_params=pltpu.CompilerParams(collective_id=0, has_side_effects=True, vmem_limit_bytes=67043328),
    )(x, dy, w_gate, w_up, w_down)


def update_kernel(dims, group, factor_ref, *refs):
    side, layers, blocks = dims
    items = len(group)
    g_refs, ins, outs, scratch = refs[:items], refs[items : items + 9], refs[-22 - 9 : -22], refs[-22:]
    g_buf, in_bufs, out_bufs, g_sem, in_sem, out_sem = scratch[0], scratch[1:10], scratch[10:19], scratch[19], scratch[20], scratch[21]
    steps = items * layers
    me = lax.axis_index("dp")
    place = (me // side, me % side)

    def window(ref, which, t):
        at = jnp.int32(0)
        for i, (c, age) in enumerate(group):
            first, by = COLOURS[c]
            at = jnp.where(t // layers == i, c * side + lax.rem(place[first] - by * age + side, side), at)
        layer = layers - 1 - lax.rem(t, layers)
        if which % 3 < 2:
            height = in_bufs[which].shape[1]
            return ref.at[layer, pl.ds(pl.multiple_of(at * height, height), height)]
        height = in_bufs[which].shape[2]
        return ref.at[layer, :, pl.ds(pl.multiple_of(at * height, height), height)]

    def load(which, t):
        slot = lax.rem(t, UPDATE_SLOTS)
        return pltpu.make_async_copy(window(ins[which], which, t), in_bufs[which].at[slot], in_sem.at[slot, which])

    def store(which, t):
        slot = lax.rem(t, UPDATE_SLOTS)
        return pltpu.make_async_copy(out_bufs[which].at[slot], window(outs[which], which, t), out_sem.at[slot, which])

    def load_g(i, t):
        slot = lax.rem(t, UPDATE_SLOTS)
        return pltpu.make_async_copy(g_refs[i].at[pl.ds(lax.rem(t, layers) * blocks, blocks)], g_buf.at[slot], g_sem.at[slot])

    def start(t):
        for i in range(items):
            @pl.when(t // layers == i)
            def _():
                load_g(i, t).start()
        for which in range(9):
            load(which, t).start()

    for t in range(min(UPDATE_SLOTS, steps)):
        start(jnp.int32(t))
    factor = factor_ref[0:1, :]

    def one(which, index, g):
        g = g.astype(F32) * factor
        m = 0.9 * in_bufs[3 + which][index] + 0.1 * g
        v = 0.95 * in_bufs[6 + which][index] + 0.05 * g * g
        w = in_bufs[which][index].astype(F32)
        out_bufs[which][index] = (w - 0.02 * (m * lax.rsqrt(v + 1e-8) + 0.1 * w)).astype(BF16)
        out_bufs[3 + which][index] = m
        out_bufs[6 + which][index] = v

    def part(t, _):
        slot = lax.rem(t, UPDATE_SLOTS)
        load_g(0, t).wait()
        for which in range(9):
            load(which, t).wait()

        @pl.when(t >= UPDATE_SLOTS)
        def _():
            for which in range(9):
                store(which, t - UPDATE_SLOTS).wait()

        for j in range(blocks):
            at = 0
            for which in range(2):
                height = in_bufs[which].shape[1]
                for i in range(BLOCK // LANES):
                    cols = slice(j * BLOCK + i * LANES, j * BLOCK + (i + 1) * LANES)
                    one(which, (slot, slice(None), cols), g_buf[slot, j, at : at + height])
                    at += height
            height, width = in_bufs[2].shape[2:]
            for i in range(width // LANES):
                one(2, (slot, j, slice(None), slice(i * LANES, (i + 1) * LANES)), g_buf[slot, j, at : at + height])
                at += height
        for which in range(9):
            store(which, t).start()

        @pl.when(t + UPDATE_SLOTS < steps)
        def _():
            start(t + UPDATE_SLOTS)
        return 0

    lax.fori_loop(0, steps, part, 0)
    for t in range(max(0, steps - UPDATE_SLOTS), steps):
        for which in range(9):
            store(which, jnp.int32(t)).wait()


def update(side, group, factor, gs, arrays, old):
    layers, d, ff = arrays[0].shape
    items, blocks = len(gs), ff // BLOCK
    chunks = len(COLOURS) * side
    arrays = [a if i % 3 < 2 else a.reshape(layers, blocks, BLOCK, d) for i, a in enumerate(arrays)]
    any_space = pl.BlockSpec(memory_space=pl.ANY)
    size = items * sum(a.size for a in arrays[:3]) // chunks
    shapes = [(UPDATE_SLOTS, d // chunks, ff)] * 2 + [(UPDATE_SLOTS, blocks, BLOCK // chunks, d)]
    bufs = [pltpu.VMEM(shapes[i % 3], a.dtype) for i, a in enumerate(arrays)]
    return pl.pallas_call(
        functools.partial(update_kernel, (side, layers, blocks), group),
        out_shape=tuple(jax.ShapeDtypeStruct(a.shape, a.dtype) for a in arrays),
        in_specs=[pl.BlockSpec(memory_space=pltpu.VMEM)] + [any_space] * (items + 9 + len(old)),
        out_specs=(any_space,) * 9,
        scratch_shapes=[
            pltpu.VMEM((UPDATE_SLOTS, blocks, *gs[0].shape[1:]), BF16), *bufs, *bufs,
            pltpu.SemaphoreType.DMA((UPDATE_SLOTS,)),
            pltpu.SemaphoreType.DMA((UPDATE_SLOTS, 9)),
            pltpu.SemaphoreType.DMA((UPDATE_SLOTS, 9)),
        ],
        input_output_aliases={1 + items + 9 + i: i for i in range(len(old))},
        compiler_params=pltpu.CompilerParams(vmem_limit_bytes=67043328),
        cost_estimate=pl.CostEstimate(flops=4000 * size, bytes_accessed=22 * size, transcendentals=size),
    )(factor, *gs, *arrays, *old)


def solution(mesh):
    n = mesh.shape["dp"]
    side = math.isqrt(n)

    def hop(c, g):
        axis, by = COLOURS[c]
        pairs = []
        for i in range(n):
            to = [i // side, i % side]
            to[axis] = (to[axis] + by) % side
            pairs.append((i, to[0] * side + to[1]))
        return lax.ppermute(g, "dp", pairs)

    def step(x, dy, *arrays):
        colours = range(len(COLOURS))
        _, factor, *parts = gradients(n, x, dy, *arrays[:3])
        parts = {(c, age): parts[age * len(COLOURS) + c] for age in range(INSIDE + 1) for c in colours}
        new = []
        for number, group in enumerate(GROUPS):
            age = INSIDE + number
            if number:
                came, new = lax.optimization_barrier(([parts[c, age] for c in colours], new))
                parts.update({(c, age): one for c, one in zip(colours, came, strict=True)})
            if age + 1 < side:
                parts.update({(c, age + 1): hop(c, parts[c, age]) for c in colours})
            new = update(side, group, factor, [parts[item] for item in group], arrays, new)
        return tuple(one.reshape(a.shape) for one, a in zip(new, arrays, strict=True))

    return jax.shard_map(
        step,
        mesh=mesh,
        in_specs=(P(("rep", "dp"), None, None),) * 2 + (P(None, None, None),) * 9,
        out_specs=(P("rep", None, None),) * 9,
        check_vma=False,
    )
```
